32 devices in a mesh: rep: 8 (over y, x, core), shard: 4 (over z).
Axes of the slice: x: 2, y: 2, z: 4, core: 2. Of those that a mesh axis runs over, the one named last changes fastest.
Arguments:
- teacher_states: bfloat16 [3072, 5120], P('rep'), may hold values from -16 to 16
- student_states: bfloat16 [3072, 3584], P('rep'), may hold values from -16 to 16
- teacher_gain: float32 [5120], replicated, may hold values from 0.25 to 1.75
- student_gain: float32 [3584], replicated, may hold values from 0.25 to 1.75
- teacher_query: bfloat16 [5120, 3072], P('rep', 'shard'), may hold values from -1 to 1
- teacher_key: bfloat16 [5120, 1024], P('rep', 'shard'), may hold values from -1 to 1
- teacher_value: bfloat16 [5120, 1024], P('rep', 'shard'), may hold values from -0.078125 to 0.078125
- teacher_output: bfloat16 [5120, 3072], P('rep', 'shard'), may hold values from -0.109375 to 0.109375
- student_query: bfloat16 [3584, 2048], P('rep', 'shard'), may hold values from -1 to 1
- student_key: bfloat16 [3584, 512], P('rep'), may hold values from -1 to 1
- student_value: bfloat16 [3584, 512], P('rep'), may hold values from -0.09375 to 0.09375
- student_output: bfloat16 [3584, 2048], P('rep', 'shard'), may hold values from -0.125 to 0.125
- projection: bfloat16 [3584, 5120], P('rep', 'shard'), may hold values from -0.09375 to 0.09375
Outputs:
- query_grad: float32 [3584, 2048], P('rep', 'shard')
- output_grad: float32 [3584, 2048], P('rep', 'shard')
The draws below stay inside these ranges and needn't reach their ends.
All inputs are finite; a program needn't handle non-finite values.
Results may differ from the reference program's by a relative error of at most 0.023.
Values may be sent and summed in bfloat16 or wider, within the bound.
A program may use at most 128 MiB of HBM per device.

```python
import math
from functools import partial
import jax
import jax.numpy as jnp
from jax import lax

D_T = 5120
HQ_T = 24
KV_T = 8
D_S = 3584
HQ_S = 16
KV_S = 4
HD = 128
SEQ = 384
TOKENS = 3072
N_REP = 8
N_SHARD = 4


def weight_matrix(key, label, rows, columns):
    folded = jax.random.fold_in(key, label)
    values = jnp.clip(jax.random.normal(folded, (rows, columns), jnp.float32), -6.0, 6.0)
    return values / math.sqrt(rows)


def drawn_states(key, label, width):
    key_noise = jax.random.fold_in(key, label)
    noise_part = jnp.clip(jax.random.normal(key_noise, (TOKENS, width), jnp.float32), -6.0, 6.0)
    return noise_part


def draw_teacher_states(key, part):
    return drawn_states(key, 11, D_T).astype(jnp.bfloat16)


def draw_student_states(key, part):
    return drawn_states(key, 21, D_S).astype(jnp.bfloat16)


def draw_teacher_query(key, part):
    return weight_matrix(key, 101, D_T, HQ_T * HD).astype(jnp.bfloat16)


def draw_teacher_key(key, part):
    return weight_matrix(key, 102, D_T, KV_T * HD).astype(jnp.bfloat16)


def draw_student_query(key, part):
    return weight_matrix(key, 201, D_S, HQ_S * HD).astype(jnp.bfloat16)


def draw_student_key(key, part):
    return weight_matrix(key, 202, D_S, KV_S * HD).astype(jnp.bfloat16)


def steps_of(key, dims, pieces, low, high):
    def one(dim, shards_of):
        heights = jax.random.uniform(jax.random.fold_in(jax.random.fold_in(key, 6), dim), (shards_of,), jnp.float32, low / len(pieces), high / len(pieces))
        return jnp.repeat(jnp.exp(heights), dims[dim] // shards_of).reshape((-1,) + (1,) * (len(dims) - dim - 1))

    level = one(*pieces[0])
    for cut in pieces[1:]:
        level = level * one(*cut)
    return level


def scatter_about(key, extent, spread, limit, cuts=(), held_as=jnp.bfloat16):
    result = spread * jax.random.normal(key, extent, jnp.float32)
    if cuts:
        result = result * steps_of(key, extent, cuts, -0.22, 0.18)
    return jnp.clip(result, -limit, limit).astype(held_as)


def setup_inputs(seed: int = 0) -> dict:
    key_of = jax.random.split(jax.random.key(seed), 14)
    return {
        "teacher_states": draw_teacher_states(jax.random.fold_in(key_of[13], 71), 0),
        "student_states": draw_student_states(jax.random.fold_in(key_of[13], 71), 0),
        "teacher_gain": jnp.clip(1.0 + 0.15 * jax.random.normal(key_of[2], (D_T,), jnp.float32), 0.25, 1.75),
        "student_gain": jnp.clip(1.0 + 0.15 * jax.random.normal(key_of[3], (D_S,), jnp.float32), 0.25, 1.75),
        "teacher_query": draw_teacher_query(jax.random.fold_in(key_of[13], 71), 0),
        "teacher_key": draw_teacher_key(jax.random.fold_in(key_of[13], 71), 0),
        "teacher_value": scatter_about(key_of[6], (D_T, KV_T * HD), D_T ** -0.5, 0.078125, ((0, 8), (1, 4))),
        "teacher_output": scatter_about(key_of[7], (D_T, HQ_T * HD), (HQ_T * HD) ** -0.5, 0.109375, ((0, 8), (1, 4))),
        "student_query": draw_student_query(jax.random.fold_in(key_of[13], 71), 0),
        "student_key": draw_student_key(jax.random.fold_in(key_of[13], 71), 0),
        "student_value": scatter_about(key_of[10], (D_S, KV_S * HD), D_S ** -0.5, 0.09375, ((0, 8),)),
        "student_output": scatter_about(key_of[11], (D_S, HQ_S * HD), (HQ_S * HD) ** -0.5, 0.125, ((0, 8), (1, 4))),
        "projection": scatter_about(key_of[12], (D_S, D_T), D_S ** -0.5, 0.09375, ((0, 8), (1, 4))),
    }


theta_base = 1000000.0
norm_epsilon = 1e-06

def rms_scale(states, gain):
    values = states.astype(jnp.float32)
    meansq = lax.optimization_barrier(jnp.mean(values * values, axis=-1, keepdims=True))
    return (values * lax.rsqrt(meansq + norm_epsilon) * gain.astype(jnp.float32)).astype(jnp.bfloat16)

def rotate(values, head_dim, turning):
    length = values.shape[0]
    halfway = head_dim // 2
    inverse = theta_base ** (-(jnp.arange(halfway, dtype=jnp.float32) * 2.0 / head_dim))
    angles = jnp.arange(length, dtype=jnp.float32)[:, None] * inverse[None, :]
    cosine = jnp.cos(angles)[:, None, :]
    sine = turning * jnp.sin(angles)[:, None, :]
    split = values.reshape(length, -1, head_dim)
    former = split[..., :halfway]
    latter = split[..., halfway:]
    turned = jnp.concatenate([former * cosine - latter * sine, latter * cosine + former * sine], axis=-1)
    return turned.reshape(length, -1)

def attend(query_rot, keys, values, head_dim):
    length = query_rot.shape[0]
    kv_heads = keys.shape[1] // head_dim
    group_size = query_rot.shape[1] // head_dim // kv_heads
    queries = query_rot.astype(jnp.bfloat16).reshape(length, kv_heads, group_size, head_dim)
    key_heads = keys.reshape(length, kv_heads, head_dim)
    value_heads = values.reshape(length, kv_heads, head_dim)
    scores = jnp.einsum('qkgd,skd->kgqs', queries, key_heads, preferred_element_type=jnp.float32) * head_dim ** (-0.5)
    rows_index = jnp.arange(length)[:, None]
    column_index = jnp.arange(length)[None, :]
    scores = jnp.where(rows_index >= column_index, scores, -1e+30)
    highest = lax.optimization_barrier(jnp.max(scores, axis=-1, keepdims=True))
    weights = jnp.exp(scores - highest)
    probs = (weights / lax.optimization_barrier(jnp.sum(weights, axis=-1, keepdims=True))).astype(jnp.bfloat16)
    mixed = jnp.einsum('kgqs,skd->qkgd', probs, value_heads, preferred_element_type=jnp.float32)
    return mixed.reshape(length, -1)

def block_sum(left, right, blocks):
    length = left.shape[0]
    width = right.shape[0]
    left_blocks = left.reshape(length, blocks, -1)
    right_blocks = right.reshape(width, blocks, -1)
    partials = jnp.einsum('snc,dnc->nsd', left_blocks, right_blocks, preferred_element_type=jnp.float32)
    rounded = lax.optimization_barrier(partials.astype(jnp.bfloat16))
    return lax.optimization_barrier(jnp.sum(rounded.astype(jnp.float32), axis=0))

def reference(teacher_states, student_states, teacher_gain, student_gain, teacher_query, teacher_key, teacher_value, teacher_output, student_query, student_key, student_value, student_output, projection):
    teacher_groups = teacher_states.reshape(N_REP, SEQ, D_T)
    student_groups = student_states.reshape(N_REP, SEQ, D_S)
    scaling = 1.0 / math.sqrt(N_REP * SEQ)

    def one_group(totals, inputs):
        teacher_rows, student_rows = inputs
        normed_t = rms_scale(teacher_rows, teacher_gain)
        query_t = rotate(jnp.dot(normed_t, teacher_query, preferred_element_type=jnp.float32), HD, 1.0)
        keys_t = rotate(jnp.dot(normed_t, teacher_key, preferred_element_type=jnp.float32), HD, 1.0).astype(jnp.bfloat16)
        values_t = jnp.dot(normed_t, teacher_value, preferred_element_type=jnp.float32).astype(jnp.bfloat16)
        mixed_t = attend(query_t, keys_t, values_t, HD).astype(jnp.bfloat16)
        attn_t = block_sum(mixed_t, teacher_output, N_SHARD)
        teacher_hidden = teacher_rows.astype(jnp.float32) + attn_t
        normed_s = rms_scale(student_rows, student_gain)
        query_s = rotate(jnp.dot(normed_s, student_query, preferred_element_type=jnp.float32), HD, 1.0)
        keys_s = rotate(jnp.dot(normed_s, student_key, preferred_element_type=jnp.float32), HD, 1.0).astype(jnp.bfloat16)
        values_s = jnp.dot(normed_s, student_value, preferred_element_type=jnp.float32).astype(jnp.bfloat16)
        mixed_full, pullback = jax.vjp(partial(attend, keys=keys_s, values=values_s, head_dim=HD), query_s)
        mixed_s = mixed_full.astype(jnp.bfloat16)
        attn_s = block_sum(mixed_s, student_output, N_SHARD)
        student_hidden = (student_rows.astype(jnp.float32) + attn_s).astype(jnp.bfloat16)
        predicted = jnp.dot(student_hidden, projection, preferred_element_type=jnp.float32)
        grad_pred = ((predicted - teacher_hidden) * scaling).astype(jnp.bfloat16)
        grad_hidden = block_sum(grad_pred, projection, N_SHARD).astype(jnp.bfloat16)
        out_term = jnp.dot(grad_hidden.T, mixed_s, preferred_element_type=jnp.float32)
        grad_mixed = jnp.dot(grad_hidden, student_output, preferred_element_type=jnp.float32)
        grad_rot = pullback(grad_mixed)[0]
        grad_query = rotate(grad_rot, HD, -1.0).astype(jnp.bfloat16)
        query_term = jnp.dot(normed_s.T, grad_query, preferred_element_type=jnp.float32)
        return ((totals[0] + query_term, totals[1] + out_term), None)
    zeros = jnp.zeros(student_query.shape, jnp.float32)
    (query_total, output_total), _ = lax.scan(one_group, (zeros, zeros), (teacher_groups, student_groups))
    return (query_total, output_total)
```

```python
from functools import partial
import math

import jax
import jax.numpy as jnp
from jax import lax
from jax.sharding import PartitionSpec as P

HQ_S = 16
KV_S = 4
HD = 128


theta_base = 1000000.0
norm_epsilon = 1e-06


def rms_scale(states, gain):
    values = states.astype(jnp.float32)
    meansq = jnp.mean(values * values, axis=-1, keepdims=True)
    return (values * lax.rsqrt(meansq + norm_epsilon) * gain).astype(jnp.bfloat16)


def rotate(values, head_dim, turning):
    length = values.shape[0]
    halfway = head_dim // 2
    inverse = theta_base ** (-(jnp.arange(halfway, dtype=jnp.float32) * 2.0 / head_dim))
    angles = jnp.arange(length, dtype=jnp.float32)[:, None] * inverse[None, :]
    cosine = jnp.cos(angles)[:, None, :]
    sine = turning * jnp.sin(angles)[:, None, :]
    split = values.reshape(length, -1, head_dim)
    former = split[..., :halfway]
    latter = split[..., halfway:]
    turned = jnp.concatenate(
        [former * cosine - latter * sine, latter * cosine + former * sine], axis=-1
    )
    return turned.reshape(length, -1)


def attend(query_rot, keys, values, head_dim):
    length = query_rot.shape[0]
    kv_heads = keys.shape[1] // head_dim
    group_size = query_rot.shape[1] // head_dim // kv_heads
    queries = query_rot.astype(jnp.bfloat16).reshape(length, kv_heads, group_size, head_dim)
    key_heads = keys.reshape(length, kv_heads, head_dim)
    value_heads = values.reshape(length, kv_heads, head_dim)
    scores = jnp.einsum(
        "qkgd,skd->kgqs", queries, key_heads, preferred_element_type=jnp.float32
    ) * head_dim ** (-0.5)
    rows_index = jnp.arange(length)[:, None]
    column_index = jnp.arange(length)[None, :]
    scores = jnp.where(rows_index >= column_index, scores, -1e30)
    highest = jnp.max(scores, axis=-1, keepdims=True)
    weights = jnp.exp(scores - highest)
    probs = (weights / jnp.sum(weights, axis=-1, keepdims=True)).astype(jnp.bfloat16)
    mixed = jnp.einsum("kgqs,skd->qkgd", probs, value_heads, preferred_element_type=jnp.float32)
    return mixed.reshape(length, -1)


def teacher_side(states, gain, query_w, key_w, value_w, output_w):
    normed = rms_scale(states, gain)
    queries = rotate(jnp.dot(normed, query_w, preferred_element_type=jnp.float32), HD, 1.0)
    keys = rotate(jnp.dot(normed, key_w, preferred_element_type=jnp.float32), HD, 1.0).astype(
        jnp.bfloat16
    )
    values = jnp.dot(normed, value_w, preferred_element_type=jnp.float32).astype(jnp.bfloat16)
    mixed = attend(queries, keys, values, HD).astype(jnp.bfloat16)
    return jnp.dot(mixed, output_w.T, preferred_element_type=jnp.float32)


def student_side(states, gain, query_w, key_w, value_w, output_w):
    normed = rms_scale(states, gain)
    queries = rotate(jnp.dot(normed, query_w, preferred_element_type=jnp.float32), HD, 1.0)
    keys = rotate(jnp.dot(normed, key_w, preferred_element_type=jnp.float32), HD, 1.0).astype(
        jnp.bfloat16
    )
    values = jnp.dot(normed, value_w, preferred_element_type=jnp.float32).astype(jnp.bfloat16)
    mixed_full, pullback = jax.vjp(partial(attend, keys=keys, values=values, head_dim=HD), queries)
    mixed = mixed_full.astype(jnp.bfloat16)
    partial_out = jnp.dot(mixed, output_w.T, preferred_element_type=jnp.float32)
    return (normed, mixed, pullback, partial_out)


def own_part(blocks, index):
    return lax.dynamic_index_in_dim(blocks, index, 0, keepdims=False)


def hop(value, axis, shift):
    count = lax.axis_size(axis)
    pairs = [(i, i + shift) for i in range(count) if 0 <= i + shift < count]
    return lax.ppermute(value, axis, pairs)


def add_rounded(left, right):
    return (left.astype(jnp.float32) + right.astype(jnp.float32)).astype(jnp.bfloat16)


def line_sum(term, axis, chunks, streams):
    count = lax.axis_size(axis)
    here = lax.axis_index(axis)
    width = term.shape[1]
    blocks = term.reshape(streams, chunks, -1, width)
    arrived = {}
    carry = {}
    for stream in range(streams):
        for shift in (1, -1):
            empty = jnp.zeros(blocks.shape[2:], term.dtype)
            arrived[stream, shift] = [empty]
            carry[stream, shift] = None
    for wave in range(chunks + count - 2):
        for stream in range(streams):
            for shift in (1, -1):
                place = here if shift == 1 else count - 1 - here
                sent = own_part(blocks[stream], jnp.clip(wave - place, 0, chunks - 1))
                if carry[stream, shift] is not None:
                    sent = add_rounded(sent, carry[stream, shift])
                came = hop(sent, axis, shift)
                carry[stream, shift] = came
                arrived[stream, shift].append(came)
    sums = []
    for stream in range(streams):
        total = blocks[stream].astype(jnp.float32)
        for shift in (1, -1):
            place = here if shift == 1 else count - 1 - here
            stacked = jnp.stack(arrived[stream, shift])
            total = total + lax.dynamic_slice_in_dim(stacked, place, chunks, 0).astype(jnp.float32)
        sums.append(total)
    return jnp.stack(sums).reshape(term.shape)


def line_scatter(term, width, axis):
    count = lax.axis_size(axis)
    here = lax.axis_index(axis)
    total = lax.dynamic_slice_in_dim(term, here * width, width, 1).astype(jnp.float32)
    carries = None
    for wave in range(count - 1):
        sends = []
        for side, shift in enumerate((1, -1)):
            target = here + shift * (count - 1 - wave)
            start = jnp.clip(target, 0, count - 1) * width
            sent = lax.dynamic_slice_in_dim(term, start, width, 1)
            if carries is not None:
                sent = add_rounded(sent, carries[side])
            sends.append(sent)
        sends = lax.optimization_barrier(tuple(sends))
        carries = [hop(sends[0], axis, 1), hop(sends[1], axis, -1)]
    for carry in carries:
        total = total + carry.astype(jnp.float32)
    return total


def halving_scatter(term, axis):
    count = lax.axis_size(axis)
    bits = count.bit_length() - 1
    here = lax.axis_index(axis)
    rows = term.shape[0] // count
    width = term.shape[1] // 2
    outs = []
    for half in range(2):
        part = term[:, half * width : (half + 1) * width].reshape((2,) * bits + (rows, width))
        left = list(range(bits - 1, -1, -1))
        order = [0] + (list(range(1, bits)) if half == 0 else list(range(bits - 1, 0, -1)))
        for bit in order:
            place = left.index(bit)
            left.remove(bit)
            mine = lax.rem(lax.div(here, 2**bit), 2)
            sent = lax.dynamic_index_in_dim(part, 1 - mine, place, keepdims=False)
            kept = lax.dynamic_index_in_dim(part, mine, place, keepdims=False)
            came = lax.ppermute(
                sent.astype(jnp.bfloat16), axis, [(i, i ^ (1 << bit)) for i in range(count)]
            )
            part = kept.astype(jnp.float32) + came.astype(jnp.float32)
        outs.append(part)
    return jnp.concatenate(outs, axis=1)


def cut(full, parts):
    pieces = []
    start = 0
    for part in parts:
        pieces.append(full[:, start : start + part.shape[1]])
        start += part.shape[1]
    return pieces


def local(
    teacher_states,
    student_states,
    teacher_gain,
    student_gain,
    teacher_query,
    teacher_key,
    teacher_value,
    teacher_output,
    student_query,
    student_key,
    student_value,
    student_output,
    projection,
):
    shard_index = lax.axis_index("shard")
    length = teacher_states.shape[0]
    local_heads = student_query.shape[1] // HD
    group_size = HQ_S // KV_S
    kv_count = max(local_heads // group_size, 1)
    kv_start = shard_index * local_heads // group_size * HD
    key_slice = lax.dynamic_slice_in_dim(student_key, kv_start, kv_count * HD, 1)
    value_slice = lax.dynamic_slice_in_dim(student_value, kv_start, kv_count * HD, 1)
    student_block = jnp.concatenate([student_query, key_slice, value_slice, student_output], axis=1)
    teacher_block = jnp.concatenate([teacher_query, teacher_key, teacher_value, teacher_output], axis=1)
    student_full = lax.all_gather(student_block, "rep", axis=0, tiled=True)
    student_full, teacher_block = lax.optimization_barrier((student_full, teacher_block))
    teacher_full = lax.all_gather(teacher_block, "rep", axis=0, tiled=True)
    teacher_full, projection = lax.optimization_barrier((teacher_full, projection))
    column_map = lax.all_gather(projection, "rep", axis=0, tiled=True)
    query_full, key_full, value_full, output_full = cut(
        student_full, (student_query, key_slice, value_slice, student_output)
    )
    teacher_partial = teacher_side(
        teacher_states,
        teacher_gain,
        *cut(teacher_full, (teacher_query, teacher_key, teacher_value, teacher_output)),
    )
    normed_s, mixed_s, pullback, student_partial = student_side(
        student_states, student_gain, query_full, key_full, value_full, output_full
    )
    block_width = column_map.shape[1]
    attn_block = line_scatter(teacher_partial.astype(jnp.bfloat16), block_width, "shard")
    attn_student = line_sum(student_partial.astype(jnp.bfloat16), "shard", 4, 2)
    own_states = lax.dynamic_slice_in_dim(teacher_states, shard_index * block_width, block_width, 1)
    teacher_hidden = own_states.astype(jnp.float32) + attn_block
    student_hidden = (student_states.astype(jnp.float32) + attn_student).astype(jnp.bfloat16)
    scaling = 1.0 / math.sqrt(lax.axis_size("rep") * length)
    predicted = lax.optimization_barrier(
        jnp.dot(student_hidden, column_map, preferred_element_type=jnp.float32)
    )
    grad_pred = ((predicted - teacher_hidden) * scaling).astype(jnp.bfloat16)
    back_term = jnp.dot(grad_pred, column_map.T, preferred_element_type=jnp.float32)
    grad_hidden = line_sum(back_term.astype(jnp.bfloat16), "shard", 4, 2).astype(jnp.bfloat16)
    grad_mixed = jnp.dot(grad_hidden, output_full, preferred_element_type=jnp.float32)
    grad_rot = pullback(grad_mixed)[0]
    grad_query = rotate(grad_rot, HD, -1.0).astype(jnp.bfloat16)
    out_term = jnp.dot(grad_hidden.T, mixed_s, preferred_element_type=jnp.float32)
    query_term = jnp.dot(normed_s.T, grad_query, preferred_element_type=jnp.float32)
    return (halving_scatter(query_term, "rep"), halving_scatter(out_term, "rep"))


def solution(mesh):
    return jax.shard_map(
        local,
        mesh=mesh,
        in_specs=(
            P("rep", None),
            P("rep", None),
            P(),
            P(),
            P("rep", "shard"),
            P("rep", "shard"),
            P("rep", "shard"),
            P("rep", "shard"),
            P("rep", "shard"),
            P("rep", None),
            P("rep", None),
            P("rep", "shard"),
            P("rep", "shard"),
        ),
        out_specs=(P("rep", "shard"), P("rep", "shard")),
        check_vma=False,
    )
```
